16 devices in a mesh: dp: 1, sp: 16 (over x, y, z, core).
Axes of the slice: x: 2, y: 2, z: 2, core: 2. Of those that a mesh axis runs over, the one named last changes fastest.
Arguments:
- x: bfloat16 [4096, 3072], P(('dp', 'sp'))
- gain: bfloat16 [3072], replicated
- wq: bfloat16 [3072, 4096], replicated
- wk: bfloat16 [3072, 4096], replicated
- wv: bfloat16 [3072, 4096], replicated
- wo: bfloat16 [4096, 3072], replicated
Outputs:
- output: bfloat16 [4096, 3072], P(('dp', 'sp'))
All inputs are finite; a program needn't handle non-finite values.
Results may differ from the reference program's by a relative error of at most 0.012.
Values are sent between devices in bfloat16 or wider.
A program may use at most 2 GiB of HBM per device.

```python
import jax
import jax.numpy as jnp
from jax import lax

ROWS = 4096
D = 3072
HEADS = 16
KV_HEADS = 16
HEAD = 256
THETA = 10000


def setup_inputs(seed: int = 0, part: int = 0) -> dict:
    kx, kn, kq, kk, kv, ko = jax.random.split(jax.random.key(seed), 6)

    def weights(key, rows, columns):
        return jax.random.normal(key, (rows, columns), jnp.float32) * rows**-0.5

    drawn = {
        "x": jax.random.normal(jax.random.fold_in(kx, part), (ROWS, D), jnp.float32),
        "gain": 1 + 0.1 * jax.random.normal(kn, (D,), jnp.float32),
        "wq": 2 * weights(kq, D, HEADS * HEAD),
        "wk": 2 * weights(kk, D, KV_HEADS * HEAD),
        "wv": 4 * weights(kv, D, KV_HEADS * HEAD),
        "wo": weights(ko, HEADS * HEAD, D),
    }
    return {k: v.astype(jnp.bfloat16) for k, v in drawn.items()}


def normed(x, gain):
    wide = x.astype(jnp.float32)
    scale = lax.rsqrt(jnp.mean(wide * wide, -1, keepdims=True) + 1e-6)
    return (wide * scale * gain.astype(jnp.float32)).astype(jnp.bfloat16)


def turned(t, place, theta):
    half = t.shape[-1] // 2
    angle = place.astype(jnp.float32)[:, None] * theta ** (-jnp.arange(half, dtype=jnp.float32) / half)
    cos, sin = jnp.cos(angle)[:, None], jnp.sin(angle)[:, None]
    a, b = t[..., :half].astype(jnp.float32), t[..., half:].astype(jnp.float32)
    return jnp.concatenate([a * cos - b * sin, b * cos + a * sin], -1).astype(jnp.bfloat16)


def matmul(a, w):
    return jnp.dot(a, w, preferred_element_type=jnp.float32).astype(jnp.bfloat16)


def einsum(form, a, b):
    return jnp.einsum(form, a.astype(jnp.float32), b.astype(jnp.float32))


def attention(q, k, v):
    scores = einsum("tgsd,ugd->gstu", q, k) * q.shape[-1] ** -0.5
    token = jnp.arange(q.shape[0])
    scores = jnp.where(token[:, None] >= token, scores, -jnp.inf)
    weights = jax.nn.softmax(scores, -1).astype(jnp.bfloat16)
    return einsum("gstu,ugd->tgsd", weights, v).astype(jnp.bfloat16)


def reference(x, gain, wq, wk, wv, wo):
    a, place = normed(x, gain), jnp.arange(ROWS)
    q = turned(matmul(a, wq).reshape(ROWS, HEADS, HEAD), place, THETA).reshape(ROWS, KV_HEADS, -1, HEAD)
    k = turned(matmul(a, wk).reshape(ROWS, KV_HEADS, HEAD), place, THETA)
    v = matmul(a, wv).reshape(ROWS, KV_HEADS, HEAD)
    seen = attention(q, k, v).reshape(ROWS, HEADS * HEAD)
    return (x.astype(jnp.float32) + jnp.dot(seen, wo, preferred_element_type=jnp.float32)).astype(jnp.bfloat16)
```

```python
import functools

import jax
import jax.numpy as jnp
from jax import lax
from jax.experimental import pallas as pl
from jax.experimental.pallas import tpu as pltpu
from jax.sharding import PartitionSpec as P

HEAD = 256
THETA = 10000
LOG2E = 1.4426950408889634
HIDDEN = -1e30
MESH = pl.DeviceIdType.MESH
OWN = 256
N = 16
D = 3072
BITS = (8, 4, 2)
ROWS = (96, 80, 80)
OFF = (0, 96, 176)
ORDER = (8, 4, 2, 9, 5, 3, 12, 6, 10, 13, 7, 11, 1, 0)
SLOTS = 3
W = 256
BK = 512


def turn(me, r):
    out = me
    for b in (8, 4, 2, 1):
        if r & b:
            out = out + b * (1 - 2 * lax.rem(lax.div(me, b), 2))
    return out


def groups(r):
    return [g for g in range(3) if not r & BITS[g]]


def height(r):
    return 2 * sum(ROWS[g] for g in groups(r))


def stage_at(r):
    return sum(height(s) for s in ORDER[: ORDER.index(r)])


STAGED = sum(height(r) for r in ORDER if r)


def dot(a, b, ca, cb):
    return lax.dot_general(a, b, (((ca,), (cb,)), ((), ())), preferred_element_type=jnp.float32)


def al(x):
    return pl.multiple_of(x, 16)


def attend_strip(g, s, off, land, q_at, vt, sc, emit):
    rows = ROWS[g]
    lo, hi = s * W // rows, (s * W + W - 1) // rows
    blocks = (hi + 1) * OWN // BK + (((hi + 1) * OWN) % BK > 0)
    clear = min(lo * OWN // BK, blocks)
    q = q_at(off + s * W)
    col = s * W + lax.broadcasted_iota(jnp.int32, (1, W), 1)
    place = sum(jnp.where(col >= i * rows, OWN - rows, 0) for i in range(lo + 1, hi + 1)) + (lo * (OWN - rows) + OFF[g]) + col

    def score(j, top, masked):
        at = pl.multiple_of(j * BK, BK)
        x = dot(land[0, pl.ds(at, BK), :], q, 1, 1)
        if masked:
            key = lax.broadcasted_iota(jnp.int32, (BK, W), 0) + at
            x = jnp.where(key <= place, x, HIDDEN)
        sc[pl.ds(at, BK), :] = x
        return jnp.maximum(top, x.reshape(BK // 8, 8, W).max(axis=0))

    top = jnp.full((8, W), HIDDEN, jnp.float32)
    top = lax.fori_loop(0, clear, lambda j, t: score(j, t, False), top)
    top = lax.fori_loop(clear, blocks, lambda j, t: score(j, t, True), top)
    e = HEAD**-0.5 * LOG2E
    top = top.max(axis=0, keepdims=True)

    def mix(j, acc):
        at = pl.multiple_of(j * BK, BK)
        p = jnp.exp2((sc[pl.ds(at, BK), :] - top) * e).astype(jnp.bfloat16)
        return acc + dot(vt[:, pl.ds(at, BK)], p, 1, 0)

    acc = lax.fori_loop(0, blocks, mix, jnp.zeros((HEAD + 8, W), jnp.float32))
    out = acc[:HEAD] * (1 / acc[HEAD : HEAD + 1])
    emit(s, out.T.astype(jnp.bfloat16))


def kernel(x_ref, gain_ref, cos_ref, sin_ref, wq, wk, wv, wo, y_ref,
           a_s, w_s, stage, land, vt, sc, ostage, oland, wo_s,
           w_sem, wo_sem, x_send, x_recv, t_send, t_recv, o_send, o_recv):
    me = lax.axis_index("sp")
    weights = (wk, wv, wq)

    barrier = pltpu.get_barrier_semaphore()
    for r in range(1, N):
        pl.semaphore_signal(barrier, inc=1, device_id=(0, turn(me, r)), device_id_type=MESH)

    count = len(ORDER)

    def fetch(t, i, slot):
        head = pl.multiple_of(turn(me, ORDER[i]) * HEAD, HEAD)
        for k in range(3):
            @pl.when(t == k)
            def _(k=k):
                pltpu.make_async_copy(weights[k].at[:, pl.ds(head, HEAD)], w_s.at[slot], w_sem.at[slot]).start()

    for i in range(SLOTS - 1):
        fetch(jnp.int32(0), i, i)

    def swap(g):
        base = 2 * OFF[g]
        return pltpu.make_async_remote_copy(
            src_ref=a_s.at[pl.ds(base, ROWS[g])], dst_ref=a_s.at[pl.ds(base + ROWS[g], ROWS[g])],
            send_sem=x_send.at[g], recv_sem=x_recv.at[g], device_id=(0, turn(me, BITS[g])), device_id_type=MESH)

    gain = gain_ref[...].astype(jnp.float32)
    for g in range(3):
        def norm(n, _, g=g):
            wide = x_ref[pl.ds(al(OFF[g] + n * 16), 16), :].astype(jnp.float32)
            scale = lax.rsqrt(jnp.mean(wide * wide, -1, keepdims=True) + 1e-6)
            a_s[pl.ds(al(2 * OFF[g] + n * 16), 16), :] = (wide * scale * gain).astype(jnp.bfloat16)
            return _
        lax.fori_loop(0, ROWS[g] // 16, norm, 0)
    pl.semaphore_wait(barrier, N - 1)
    for g in range(3):
        swap(g).start()
    for g in range(3):
        swap(g).wait()

    def place(t, owner, g):
        q = lax.div(t, 2)
        return al((1 - q) * (owner * OWN + OFF[g]) + q * (N * OFF[g] + owner * ROWS[g]))

    def send(t, i, only):
        r = ORDER[i]
        q, at = lax.div(t, 2), stage_at(r)
        for g in groups(r):
            if only(g):
                for owner in (me, turn(me, BITS[g])):
                    pltpu.make_async_remote_copy(
                        src_ref=stage.at[t, pl.ds(at, ROWS[g])],
                        dst_ref=land.at[t, pl.ds(place(t, owner, g), ROWS[g])],
                        send_sem=t_send.at[t], recv_sem=t_recv.at[t + q * g], device_id=(0, turn(me, r)), device_id_type=MESH).start()
                    at += ROWS[g]
            else:
                at += 2 * ROWS[g]

    def sends(t, i):
        @pl.when(t < 2)
        def _():
            send(t, i, lambda g: True)

        @pl.when(t == 2)
        def _():
            send(t, i, lambda g: g == 0)

    def project(t, _):
        plain = t == 1
        for i, r in enumerate(ORDER):
            n = t * count + i
            slot = lax.rem(n, SLOTS)
            pltpu.make_async_copy(wk.at[:, pl.ds(0, HEAD)], w_s.at[slot], w_sem.at[slot]).wait()
            ahead = i + SLOTS - 1
            after = lax.rem(n + SLOTS - 1, SLOTS)
            fetch(t + ahead // count, ahead % count, after)
            if i > 0:
                sends(t, i - 1)
            at = stage_at(r)
            for g in groups(r):
                base, rows = 2 * OFF[g], 2 * ROWS[g]
                y = dot(a_s[base : base + rows, :], w_s[slot], 1, 0).astype(jnp.bfloat16).astype(jnp.float32)
                c = jnp.where(plain, 1.0, cos_ref[base : base + rows, :])
                s = jnp.where(plain, 0.0, sin_ref[base : base + rows, :])
                u, v = y[:, : HEAD // 2], y[:, HEAD // 2 :]
                y = jnp.concatenate([u * c - v * s, v * c + u * s], 1).astype(jnp.bfloat16)
                if r:
                    stage[t, at : at + rows, :] = y
                    at += rows
                else:
                    land[t, pl.ds(place(t, me, g), ROWS[g]), :] = y[: ROWS[g]]
                    land[t, pl.ds(place(t, turn(me, BITS[g]), g), ROWS[g]), :] = y[ROWS[g] :]
        return _

    lax.fori_loop(0, 3, project, 0)
    for g in (1, 2):
        for i in range(count - 1):
            send(2, i, lambda k: k == g)
    for i in range(4):
        pltpu.make_async_copy(wo.at[pl.ds(i * 1024, 1024)], wo_s.at[pl.ds(i * 1024, 1024)], wo_sem.at[i]).start()

    def arrived(t, sem, rows):
        pltpu.make_async_copy(land.at[t, pl.ds(0, rows)], land.at[t, pl.ds(0, rows)], t_recv.at[sem]).wait()

    arrived(0, 0, 14 * OWN)
    arrived(1, 1, 14 * OWN)
    vt[HEAD:, :] = jnp.ones((8, N * OWN), jnp.bfloat16)
    for j in range(N):
        vt[:HEAD, j * OWN : (j + 1) * OWN] = land[1, j * OWN : (j + 1) * OWN, :].T

    for g in range(3):
        off = N * OFF[g]
        arrived(2, 2 + g, 14 * ROWS[g])

        def emit(s, out, off=off):
            ostage[off + s * W : off + (s + 1) * W, :] = out

        for s in range(N * ROWS[g] // W):
            attend_strip(g, s, off, land, lambda at: land[2, at : at + W, :], vt, sc, emit)
        mine = pl.ds(pl.multiple_of(me * HEAD, HEAD), HEAD)
        for r in ORDER[:-1] + (14, 15):
            to = turn(me, r)
            pltpu.make_async_remote_copy(
                src_ref=ostage.at[pl.ds(al(off + to * ROWS[g]), ROWS[g])], dst_ref=oland.at[pl.ds(OFF[g], ROWS[g]), mine],
                send_sem=o_send.at[g], recv_sem=o_recv.at[g], device_id=(0, to), device_id_type=MESH).start()
        oland[OFF[g] : OFF[g] + ROWS[g], mine] = ostage[pl.ds(al(off + me * ROWS[g]), ROWS[g]), :]

    for i in range(4):
        pltpu.make_async_copy(wo.at[pl.ds(i * 1024, 1024)], wo_s.at[pl.ds(i * 1024, 1024)], wo_sem.at[i]).wait()
    for g in range(3):
        rows = slice(OFF[g], OFF[g] + ROWS[g])
        part = ostage.at[pl.ds(0, 15 * ROWS[g])]
        pltpu.make_async_copy(part, part, o_recv.at[g]).wait()

        def out(n, _, rows=rows):
            cols = pl.ds(pl.multiple_of(n * 512, 512), 512)
            y = dot(oland[rows, :], wo_s[:, cols], 1, 0)
            y_ref[rows, cols] = (x_ref[rows, cols].astype(jnp.float32) + y).astype(jnp.bfloat16)
            return _
        lax.fori_loop(0, D // 512, out, 0)

    for t in range(3):
        whole = stage.at[t]
        pltpu.make_async_copy(whole, whole, t_send.at[t]).wait()
    for g in range(3):
        part = ostage.at[pl.ds(0, 15 * ROWS[g])]
        pltpu.make_async_copy(part, part, o_send.at[g]).wait()


def solution(mesh):
    def step(x, gain, wq, wk, wv, wo):
        me = lax.axis_index("sp")
        own = [OFF[g] + jnp.arange(ROWS[g]) for g in range(3)]
        place = jnp.concatenate([p for g in range(3) for p in (me * OWN + own[g], (me ^ BITS[g]) * OWN + own[g])])
        half = HEAD // 2
        angle = place.astype(jnp.float32)[:, None] * THETA ** (-jnp.arange(half, dtype=jnp.float32) / half)
        vmem, any_ = pl.BlockSpec(memory_space=pltpu.VMEM), pl.BlockSpec(memory_space=pl.ANY)
        bf, f32 = jnp.bfloat16, jnp.float32
        dma = pltpu.SemaphoreType.DMA
        return pl.pallas_call(
            kernel,
            out_shape=jax.ShapeDtypeStruct((OWN, D), bf),
            in_specs=[vmem] * 4 + [any_] * 4,
            out_specs=vmem,
            scratch_shapes=[
                pltpu.VMEM((2 * OWN, D), bf), pltpu.VMEM((SLOTS, D, HEAD), bf), pltpu.VMEM((3, STAGED, HEAD), bf),
                pltpu.VMEM((3, N * OWN, HEAD), bf), pltpu.VMEM((HEAD + 8, N * OWN), bf), pltpu.VMEM((N * OWN, W), f32),
                pltpu.VMEM((N * OWN, HEAD), bf), pltpu.VMEM((OWN, N * HEAD), bf), pltpu.VMEM((N * HEAD, D), bf),
                dma((SLOTS,)), dma((4,)), dma((3,)), dma((3,)), dma((3,)), dma((5,)), dma((3,)), dma((3,)),
            ],
            compiler_params=pltpu.CompilerParams(collective_id=0, has_side_effects=True, vmem_limit_bytes=67_043_328),
            name="layer",
        )(x, gain[None], jnp.cos(angle), jnp.sin(angle), wq, wk, wv, wo)

    tokens, whole = P(("dp", "sp"), None), P(None, None)
    return jax.shard_map(step, mesh=mesh, in_specs=(tokens, P(None), whole, whole, whole, whole), out_specs=tokens, check_vma=False)
```

```python
import functools

import jax
import jax.numpy as jnp
from jax import lax
from jax.experimental import pallas as pl
from jax.experimental.pallas import tpu as pltpu
from jax.sharding import PartitionSpec as P

HEAD = 256
THETA = 10000
LOG2E = 1.4426950408889634
HIDDEN = -1e30
MESH = pl.DeviceIdType.MESH
OWN = 256
N = 16
D = 3072
BITS = (8, 4, 2)
ROWS = (96, 80, 80)
OFF = (0, 96, 176)
ORDER = (8, 4, 2, 12, 6, 10, 0)
SLOTS = 4
W = 256


def turn(me, r):
    out = me
    for b in (8, 4, 2, 1):
        if r & b:
            out = out + b * (1 - 2 * lax.rem(lax.div(me, b), 2))
    return out


def groups(r):
    return [g for g in range(3) if not r & BITS[g]]


def height(r):
    return 2 * sum(ROWS[g] for g in groups(r))


def stage_at(r):
    return sum(2 * height(s) for s in ORDER[: ORDER.index(r)])


def dot(a, b, ca, cb):
    return lax.dot_general(a, b, (((ca,), (cb,)), ((), ())), preferred_element_type=jnp.float32)


def al(x):
    return pl.multiple_of(x, 16)


def attend_strip(g, s, q, k_ref, vt):
    rows = ROWS[g]
    lo, hi = s * W // rows, (s * W + W - 1) // rows
    clear, keys = lo * OWN, (hi + 1) * OWN
    col = s * W + lax.broadcasted_iota(jnp.int32, (1, W), 1)
    place = sum(jnp.where(col >= i * rows, OWN - rows, 0) for i in range(lo + 1, hi + 1)) + (lo * (OWN - rows) + OFF[g]) + col
    key = lax.broadcasted_iota(jnp.int32, (keys - clear, W), 0) + clear
    x = jnp.where(key <= place, dot(k_ref[clear:keys, :], q, 1, 1), HIDDEN)
    if clear:
        x = jnp.concatenate([dot(k_ref[:clear, :], q, 1, 1), x], axis=0)
    top = x.max(axis=0, keepdims=True)
    p = jnp.exp2((x - top) * (HEAD**-0.5 * LOG2E)).astype(jnp.bfloat16)
    acc = dot(vt[:, :keys], p, 1, 0)
    out = acc[:HEAD] * (1 / acc[HEAD : HEAD + 1])
    return out.T.astype(jnp.bfloat16)


def kernel(x_ref, gain_ref, cos_ref, sin_ref, wq, wk, wv, wo, y_ref,
           a_s, stage, land, vt, ostage, oland,
           w_sem, wo_sem, x_send, x_recv, t_send, t_recv, o_send, o_recv):
    me = lax.axis_index("sp")
    side = lax.rem(me, 2)
    weights = (wk, wv, wq)
    count = len(ORDER)

    barrier = pltpu.get_barrier_semaphore()
    for r in range(1, N):
        pl.semaphore_signal(barrier, inc=1, device_id=(0, turn(me, r)), device_id_type=MESH)

    def place(t, owner, g):
        q = lax.div(t, 2)
        return al((1 - q) * (owner * OWN + OFF[g]) + q * (N * OFF[g] + owner * ROWS[g]))

    def send(t, i, only):
        r = ORDER[i]
        q = lax.div(t, 2)
        for p in range(2 if r else 1):
            at = stage_at(r) + (p if r else 1 - side) * height(r)
            to = turn(me, r) - side + p if r else turn(me, 1)
            for g in groups(r):
                for owner in (me, turn(me, BITS[g])):
                    if only(g):
                        pltpu.make_async_remote_copy(
                            src_ref=stage.at[t, pl.ds(al(at), ROWS[g])],
                            dst_ref=land.at[t, pl.ds(place(t, owner, g), ROWS[g])],
                            send_sem=t_send.at[t], recv_sem=t_recv.at[t + q * g], device_id=(0, to), device_id_type=MESH).start()
                    at += ROWS[g]

    def sends(t, i):
        @pl.when(t < 2)
        def _():
            send(t, i, lambda g: True)

        @pl.when(t == 2)
        def _():
            send(t, i, lambda g: g == 0)

    def front(w_s):
        def fetch(t, i, slot):
            head = pl.multiple_of((turn(me, ORDER[i]) - side) * HEAD, 2 * HEAD)
            for k in range(3):
                @pl.when(t == k)
                def _(k=k):
                    pltpu.make_async_copy(weights[k].at[:, pl.ds(head, 2 * HEAD)], w_s.at[slot], w_sem.at[slot]).start()

        for i in range(SLOTS - 1):
            fetch(jnp.int32(0), i, i)

        def swap(g):
            base = 2 * OFF[g]
            return pltpu.make_async_remote_copy(
                src_ref=a_s.at[pl.ds(base, ROWS[g])], dst_ref=a_s.at[pl.ds(base + ROWS[g], ROWS[g])],
                send_sem=x_send.at[g], recv_sem=x_recv.at[g], device_id=(0, turn(me, BITS[g])), device_id_type=MESH)

        gain = gain_ref[...].astype(jnp.float32)
        for g in range(3):
            def norm(n, _, g=g):
                wide = x_ref[pl.ds(al(OFF[g] + n * 16), 16), :].astype(jnp.float32)
                scale = lax.rsqrt(jnp.mean(wide * wide, -1, keepdims=True) + 1e-6)
                a_s[pl.ds(al(2 * OFF[g] + n * 16), 16), :] = (wide * scale * gain).astype(jnp.bfloat16)
                return _
            lax.fori_loop(0, ROWS[g] // 16, norm, 0)
        pl.semaphore_wait(barrier, N - 1)
        for g in range(3):
            swap(g).start()
        for g in range(3):
            swap(g).wait()

        def project(t, _):
            plain = t == 1
            for i, r in enumerate(ORDER):
                n = t * count + i
                slot = lax.rem(n, SLOTS)
                pltpu.make_async_copy(wk.at[:, pl.ds(0, 2 * HEAD)], w_s.at[slot], w_sem.at[slot]).wait()
                ahead = i + SLOTS - 1
                fetch(t + ahead // count, ahead % count, lax.rem(n + SLOTS - 1, SLOTS))
                if i > 0:
                    sends(t, i - 1)
                cuts = [slice(2 * OFF[g], 2 * OFF[g] + 2 * ROWS[g]) for g in groups(r)]
                rows = lambda ref: jnp.concatenate([ref[c, :] for c in cuts], axis=0)
                y = dot(rows(a_s), w_s[slot], 1, 0).astype(jnp.bfloat16).astype(jnp.float32)
                cos, sin = jnp.where(plain, 1.0, rows(cos_ref)), jnp.where(plain, 0.0, rows(sin_ref))
                for p in range(2):
                    u, v = y[:, p * HEAD : p * HEAD + HEAD // 2], y[:, p * HEAD + HEAD // 2 : (p + 1) * HEAD]
                    at = stage_at(r) + p * height(r)
                    stage[t, at : at + height(r), :] = jnp.concatenate([u * cos - v * sin, v * cos + u * sin], 1).astype(jnp.bfloat16)
            sends(t, count - 1)
            at = stage_at(0) + side * height(0)
            for g in range(3):
                for owner in (me, turn(me, BITS[g])):
                    land[t, pl.ds(place(t, owner, g), ROWS[g]), :] = stage[t, pl.ds(al(at), ROWS[g]), :]
                    at += ROWS[g]
            return _

        lax.fori_loop(0, 3, project, 0)
        for g in (1, 2):
            for i in range(count):
                send(2, i, lambda k: k == g)

    pl.run_scoped(front, pltpu.VMEM((SLOTS, D, 2 * HEAD), jnp.bfloat16))

    def back(wo_s):
        def load(i):
            return pltpu.make_async_copy(wo.at[pl.ds(i * 1024, 1024)], wo_s.at[pl.ds(i * 1024, 1024)], wo_sem.at[i])

        for i in range(4):
            load(i).start()

        def arrived(t, sem, rows):
            pltpu.make_async_copy(land.at[t, pl.ds(0, rows)], land.at[t, pl.ds(0, rows)], t_recv.at[sem]).wait()

        arrived(0, 0, 14 * OWN)
        arrived(1, 1, 14 * OWN)
        vt[HEAD:, :] = jnp.ones((8, N * OWN), jnp.bfloat16)
        for j in range(N):
            vt[:HEAD, j * OWN : (j + 1) * OWN] = land[1, j * OWN : (j + 1) * OWN, :].T

        for g in range(3):
            off = N * OFF[g]
            arrived(2, 2 + g, 14 * ROWS[g])
            for s in range(N * ROWS[g] // W):
                at = slice(off + s * W, off + (s + 1) * W)
                ostage[at, :] = attend_strip(g, s, land[2, at, :], land.at[0], vt)
            mine = pl.ds(pl.multiple_of(me * HEAD, HEAD), HEAD)
            for r in (8, 4, 2, 9, 5, 3, 12, 6, 10, 13, 7, 11, 14, 15, 1):
                to = turn(me, r)
                pltpu.make_async_remote_copy(
                    src_ref=ostage.at[pl.ds(al(off + to * ROWS[g]), ROWS[g])], dst_ref=oland.at[pl.ds(OFF[g], ROWS[g]), mine],
                    send_sem=o_send.at[g], recv_sem=o_recv.at[g], device_id=(0, to), device_id_type=MESH).start()
            oland[OFF[g] : OFF[g] + ROWS[g], mine] = ostage[pl.ds(al(off + me * ROWS[g]), ROWS[g]), :]

        for i in range(4):
            load(i).wait()
        for gs, rows in (((0, 1), slice(0, OFF[2])), ((2,), slice(OFF[2], OWN))):
            for g in gs:
                part = ostage.at[pl.ds(0, 15 * ROWS[g])]
                pltpu.make_async_copy(part, part, o_recv.at[g]).wait()

            def out(n, _, rows=rows):
                cols = pl.ds(pl.multiple_of(n * 1024, 1024), 1024)
                y = dot(oland[rows, :], wo_s[:, cols], 1, 0)
                y_ref[rows, cols] = (x_ref[rows, cols].astype(jnp.float32) + y).astype(jnp.bfloat16)
                return _
            lax.fori_loop(0, D // 1024, out, 0)

    pl.run_scoped(back, pltpu.VMEM((N * HEAD, D), jnp.bfloat16))

    for t in range(3):
        part = stage.at[t, pl.ds(0, 14 * OWN)]
        pltpu.make_async_copy(part, part, t_send.at[t]).wait()
    for g in range(3):
        part = ostage.at[pl.ds(0, 15 * ROWS[g])]
        pltpu.make_async_copy(part, part, o_send.at[g]).wait()


def solution(mesh):
    def step(x, gain, wq, wk, wv, wo):
        me = lax.axis_index("sp")
        own = [OFF[g] + jnp.arange(ROWS[g]) for g in range(3)]
        place = jnp.concatenate([p for g in range(3) for p in (me * OWN + own[g], (me ^ BITS[g]) * OWN + own[g])])
        half = HEAD // 2
        angle = place.astype(jnp.float32)[:, None] * THETA ** (-jnp.arange(half, dtype=jnp.float32) / half)
        vmem, any_ = pl.BlockSpec(memory_space=pltpu.VMEM), pl.BlockSpec(memory_space=pl.ANY)
        bf = jnp.bfloat16
        dma = pltpu.SemaphoreType.DMA
        return pl.pallas_call(
            kernel,
            out_shape=jax.ShapeDtypeStruct((OWN, D), bf),
            in_specs=[vmem] * 4 + [any_] * 4,
            out_specs=vmem,
            scratch_shapes=[
                pltpu.VMEM((2 * OWN, D), bf), pltpu.VMEM((3, N * OWN, HEAD), bf), pltpu.VMEM((3, N * OWN, HEAD), bf),
                pltpu.VMEM((HEAD + 8, N * OWN), bf), pltpu.VMEM((N * OWN, HEAD), bf), pltpu.VMEM((OWN, N * HEAD), bf),
                dma((SLOTS,)), dma((4,)), dma((3,)), dma((3,)), dma((3,)), dma((5,)), dma((3,)), dma((3,)),
            ],
            compiler_params=pltpu.CompilerParams(collective_id=0, has_side_effects=True, vmem_limit_bytes=67_043_328),
            name="layer",
        )(x, gain[None], jnp.cos(angle), jnp.sin(angle), wq, wk, wv, wo)

    tokens, whole = P(("dp", "sp"), None), P(None, None)
    return jax.shard_map(step, mesh=mesh, in_specs=(tokens, P(None), whole, whole, whole, whole), out_specs=tokens, check_vma=False)
```

```python
import jax
import jax.numpy as jnp
import numpy as np
from jax import lax
from jax.experimental import pallas as pl
from jax.experimental.pallas import tpu as pltpu
from jax.sharding import PartitionSpec as P

HEAD = 256
THETA = 10000
LOG2E = 1.4426950408889634
HIDDEN = -1e30
MESH = pl.DeviceIdType.MESH
OWN = 256
N = 16
D = 3072
BITS = (8, 4, 2)
PIECES = ((32, 32, 32), (32, 32, 16), (32, 16, 32))
ROWS = tuple(sum(p) for p in PIECES)
OFF = tuple(sum(ROWS[:g]) for g in range(3))
LONG = tuple(sum(p[c] for p in PIECES) for c in range(3))
AT = tuple(sum(LONG[:c]) for c in range(3))
ORDER = (8, 4, 2, 12, 6, 10, 0)
SLOTS = 4
W = 256
WINDOWS = (20, 20, 20, 20, 40, 40)


def turn(me, r):
    out = me
    for b in (8, 4, 2, 1):
        if r & b:
            out = out + b * (1 - 2 * lax.rem(lax.div(me, b), 2))
    return out


def groups(r):
    return [g for g in range(3) if not r & BITS[g]]


def height(r):
    return 2 * sum(ROWS[g] for g in groups(r))


def stage_at(r):
    return sum(2 * height(s) for s in ORDER[: ORDER.index(r)])


def token(g, c):
    return AT[c] + sum(PIECES[h][c] for h in range(g))


def inside(g, c):
    return sum(PIECES[g][:c])


TOKENS = np.concatenate([token(g, c) + np.arange(PIECES[g][c]) for g in range(3) for c in range(3)])


def dot(a, b, ca, cb):
    return lax.dot_general(a, b, (((ca,), (cb,)), ((), ())), preferred_element_type=jnp.float32)


def al(x):
    return pl.multiple_of(x, 16)


def attend_strip(rows, first, s, q, k_ref, vt, order_ref):
    lo, hi = s * W // rows, (s * W + W - 1) // rows
    clear, keys = lo * OWN, (hi + 1) * OWN
    col = s * W + lax.broadcasted_iota(jnp.int32, (1, W), 1)
    place = sum(jnp.where(col >= i * rows, OWN - rows, 0) for i in range(lo + 1, hi + 1)) + (lo * (OWN - rows) + first) + col
    x = dot(k_ref[clear:keys, :], q, 1, 1)
    x = jnp.concatenate(
        [jnp.where(order_ref[...] <= place - (lo + n) * OWN, x[n * OWN : (n + 1) * OWN], HIDDEN) for n in range(hi - lo + 1)], axis=0)
    if clear:
        x = jnp.concatenate([dot(k_ref[:clear, :], q, 1, 1), x], axis=0)
    top = x.max(axis=0, keepdims=True)
    p = jnp.exp2((x - top) * (HEAD**-0.5 * LOG2E)).astype(jnp.bfloat16)
    acc = dot(vt[:, :keys], p, 1, 0)
    out = acc[:HEAD] * (1 / acc[HEAD : HEAD + 1])
    return out.T.astype(jnp.bfloat16)


def rows_of(phase, i):
    r = ORDER[i]
    heads = 2 if r else 1
    if phase < 3:
        return heads * sum(ROWS[g] for g in groups(r)) * (2 if phase == 2 else 1)
    return heads * 2 * sum(PIECES[g][phase - 3] for g in groups(r))


COUNT = len(ORDER)
UNITS = [(phase, i) for phase in range(6) for i in range(COUNT) if rows_of(phase, i)]
BEFORE = {}
seen = 0
for at, unit in enumerate(UNITS):
    BEFORE[unit] = UNITS[seen : max(at - WINDOWS[unit[0]], seen)]
    seen += len(BEFORE[unit])
LEFT = UNITS[seen:]


def kernel(gain_ref, turn_ref, base_ref, order_ref, x, wq, wk, wv, wo, y,
           x_s, y_s, cos_s, sin_s, a_s, stage, land, vt, ostage, oland,
           w_sem, wo_sem, x_sem, y_sem, x_send, x_recv, t_send, t_recv, o_send, o_recv):
    me = lax.axis_index("sp")
    side = lax.rem(me, 2)
    weights = (wk, wv, wq)

    read = pltpu.make_async_copy(x, x_s, x_sem)
    read.start()
    barrier = pltpu.get_barrier_semaphore()
    for r in range(1, N):
        pl.semaphore_signal(barrier, inc=1, device_id=(0, turn(me, r)), device_id_type=MESH)

    def blocks(t, owner, g):
        if t < 2:
            return [(0, ROWS[g], al(owner * OWN + OFF[g]), None)]
        return [(inside(g, c), PIECES[g][c], al(N * AT[c] + owner * LONG[c] + token(g, c) - AT[c]), c) for c in range(3)]

    def sent(unit):
        part = stage.at[0, pl.ds(0, rows_of(*unit))]
        pltpu.make_async_copy(part, part, t_send.at[unit[0], unit[1]]).wait()

    def send(phase, i):
        if not rows_of(phase, i):
            return
        for unit in BEFORE[phase, i]:
            sent(unit)
        r, t = ORDER[i], (0, 0, 1, 2, 2, 2)[phase]
        for p in range(2 if r else 1):
            at = stage_at(r) + (p if r else 1 - side) * height(r)
            to = turn(me, r) - side + p if r else turn(me, 1)
            for g in groups(r):
                for n, owner in enumerate((me, turn(me, BITS[g]))):
                    for skip, rows, to_row, c in blocks(t, owner, g):
                        if phase < 2 and n == phase or phase == 2 or phase > 2 and phase - 3 == c:
                            pltpu.make_async_remote_copy(
                                src_ref=stage.at[t, pl.ds(al(at + skip), rows)], dst_ref=land.at[t, pl.ds(to_row, rows)],
                                send_sem=t_send.at[phase, i], recv_sem=t_recv.at[t + max(phase - 3, 0)], device_id=(0, to),
                                device_id_type=MESH).start()
                    at += ROWS[g]

    def front(w_s):
        def fetch(step, i, slot):
            head = pl.multiple_of((turn(me, ORDER[i]) - side) * HEAD, 2 * HEAD)
            for k, is_k in enumerate((step < 2, step == 2, step == 3)):
                @pl.when(is_k)
                def _(k=k):
                    pltpu.make_async_copy(weights[k].at[:, pl.ds(head, 2 * HEAD)], w_s.at[slot], w_sem.at[slot]).start()

        for i in range(SLOTS - 1):
            fetch(jnp.int32(0), i, i)

        def swap(g):
            base = 2 * OFF[g]
            return pltpu.make_async_remote_copy(
                src_ref=a_s.at[pl.ds(base, ROWS[g])], dst_ref=a_s.at[pl.ds(base + ROWS[g], ROWS[g])],
                send_sem=x_send.at[g], recv_sem=x_recv.at[g], device_id=(0, turn(me, BITS[g])), device_id_type=MESH)

        gain = gain_ref[...].astype(jnp.float32).reshape(1, D)
        read.wait()
        for g in range(3):
            for n in range(ROWS[g] // 16):
                at = int(TOKENS[OFF[g] + n * 16])
                wide = x_s[at : at + 16, :].astype(jnp.float32)
                scale = lax.rsqrt(jnp.mean(wide * wide, -1, keepdims=True) + 1e-6)
                a_s[2 * OFF[g] + n * 16 : 2 * OFF[g] + n * 16 + 16, :] = (wide * scale * gain).astype(jnp.bfloat16)
            if g == 0:
                pl.semaphore_wait(barrier, N - 1)
            else:
                swap(g - 1).start()
        swap(2).start()

        for g in range(3):
            for n, owner in enumerate((me, turn(me, BITS[g]))):
                cb, sb = base_ref[owner, :, : HEAD // 2], base_ref[owner, :, HEAD // 2 :]
                ct, st = turn_ref[OFF[g] : OFF[g] + ROWS[g], : HEAD // 2], turn_ref[OFF[g] : OFF[g] + ROWS[g], HEAD // 2 :]
                at = slice(2 * OFF[g] + n * ROWS[g], 2 * OFF[g] + (n + 1) * ROWS[g])
                cos_s[at, :] = cb * ct - sb * st
                sin_s[at, :] = sb * ct + cb * st

        def next_weights(step, i):
            n = step * COUNT + i
            slot = lax.rem(n, SLOTS)
            pltpu.make_async_copy(wk.at[:, pl.ds(0, 2 * HEAD)], w_s.at[slot], w_sem.at[slot]).wait()
            ahead = i + SLOTS - 1
            fetch(step + ahead // COUNT, ahead % COUNT, lax.rem(n + SLOTS - 1, SLOTS))
            return w_s[slot]

        def rotated(y, cos, sin):
            u, v = y[:, : HEAD // 2], y[:, HEAD // 2 :]
            return jnp.concatenate([u * cos - v * sin, v * cos + u * sin], 1).astype(jnp.bfloat16)

        def half(which, carry):
            @pl.when(which == 1)
            def _():
                for g in range(3):
                    swap(g).wait()

            def sends(i):
                for k in range(2):
                    @pl.when(which == k)
                    def _(k=k):
                        send(k, i)

            for i, r in enumerate(ORDER):
                w = next_weights(which, i)
                if i > 0:
                    sends(i - 1)
                rows = lambda ref: jnp.concatenate(
                    [ref[pl.ds(al(2 * OFF[g] + which * ROWS[g]), ROWS[g]), :] for g in groups(r)], axis=0)
                y = dot(rows(a_s), w, 1, 0).astype(jnp.bfloat16).astype(jnp.float32)
                cos, sin = rows(cos_s), rows(sin_s)
                for p in range(2):
                    z = rotated(y[:, p * HEAD : (p + 1) * HEAD], cos, sin)
                    at, n = stage_at(r) + p * height(r), 0
                    for g in groups(r):
                        stage[0, pl.ds(al(at + which * ROWS[g]), ROWS[g]), :] = z[n : n + ROWS[g]]
                        at, n = at + 2 * ROWS[g], n + ROWS[g]
            sends(COUNT - 1)
            return carry

        lax.fori_loop(0, 2, half, 0)

        def project(t, carry):
            plain = t == 1

            def sends(i):
                for k in (1, 2):
                    @pl.when(t == k)
                    def _(k=k):
                        send(k + 1, i)

            for i, r in enumerate(ORDER):
                w = next_weights(t + 1, i)
                if i > 0:
                    sends(i - 1)
                cuts = [slice(2 * OFF[g], 2 * OFF[g] + 2 * ROWS[g]) for g in groups(r)]
                rows = lambda ref: jnp.concatenate([ref[c, :] for c in cuts], axis=0)
                y = dot(rows(a_s), w, 1, 0).astype(jnp.bfloat16).astype(jnp.float32)
                cos, sin = jnp.where(plain, 1.0, rows(cos_s)), jnp.where(plain, 0.0, rows(sin_s))
                for p in range(2):
                    at = stage_at(r) + p * height(r)
                    stage[t, at : at + height(r), :] = rotated(y[:, p * HEAD : (p + 1) * HEAD], cos, sin)
            sends(COUNT - 1)
            return carry

        lax.fori_loop(1, 3, project, 0)

    pl.run_scoped(front, pltpu.VMEM((SLOTS, D, 2 * HEAD), jnp.bfloat16))

    def back(wo_s):
        for i in range(COUNT):
            send(4, i)

        def load(i):
            return pltpu.make_async_copy(wo.at[pl.ds(i * 1024, 1024)], wo_s.at[pl.ds(i * 1024, 1024)], wo_sem.at[i])

        for i in range(4):
            load(i).start()

        def arrived(t, sem, rows):
            pltpu.make_async_copy(land.at[t, pl.ds(0, rows)], land.at[t, pl.ds(0, rows)], t_recv.at[sem]).wait()

        for t in range(3):
            at = stage_at(0) + side * height(0)
            for g in range(3):
                for owner in (me, turn(me, BITS[g])):
                    for skip, rows, to_row, _ in blocks(t, owner, g):
                        land[t, pl.ds(to_row, rows), :] = stage[t, pl.ds(al(at + skip), rows), :]
                    at += ROWS[g]
        vt[HEAD:, :] = jnp.ones((8, N * OWN), jnp.bfloat16)
        arrived(0, 0, 14 * OWN)
        arrived(1, 1, 14 * OWN)
        for j in range(N):
            vt[:HEAD, j * OWN : (j + 1) * OWN] = land[1, j * OWN : (j + 1) * OWN, :].T

        mine = pl.ds(pl.multiple_of(me * HEAD, HEAD), HEAD)

        def attend(c, rows, first, between):
            arrived(2, 2 + c, 14 * rows)
            for s in range(N * rows // W):
                at = pl.ds(al(N * first + s * W), W)
                ostage[at, :] = attend_strip(rows, first, s, land[2, at, :], land.at[0], vt, order_ref)
                between(s)
            for r in (8, 4, 2, 9, 5, 3, 12, 6, 10, 13, 7, 11, 14, 15, 1):
                to = turn(me, r)
                pltpu.make_async_remote_copy(
                    src_ref=ostage.at[pl.ds(al(N * first + to * rows), rows)], dst_ref=oland.at[pl.ds(al(first), rows), mine],
                    send_sem=o_send.at[c], recv_sem=o_recv.at[c], device_id=(0, to), device_id_type=MESH).start()
            oland[pl.ds(al(first), rows), mine] = ostage[pl.ds(al(N * first + me * rows), rows), :]

        def last_queries(s):
            for i in range(COUNT * s // 5, min(COUNT * (s + 1) // 5, COUNT)):
                send(5, i)

        attend(0, LONG[0], 0, last_queries)

        def rest(c, carry):
            attend(c, LONG[1], AT[1] + (c - 1) * LONG[1], lambda s: None)
            return carry

        lax.fori_loop(1, 3, rest, 0)

        for i in range(4):
            load(i).wait()

        def project(c, rows, first):
            part = ostage.at[pl.ds(0, 15 * rows)]
            pltpu.make_async_copy(part, part, o_recv.at[c]).wait()
            own = pl.ds(al(first), rows)

            def out(n, carry):
                cols = pl.ds(pl.multiple_of(n * 512, 512), 512)
                z = dot(oland[own, :], wo_s[:, cols], 1, 0)
                y_s[own, cols] = (x_s[own, cols].astype(jnp.float32) + z).astype(jnp.bfloat16)
                return carry

            lax.fori_loop(0, D // 512, out, 0)
            pltpu.make_async_copy(y_s.at[own], y.at[own], y_sem.at[c]).start()

        project(0, LONG[0], 0)

        def project_rest(c, carry):
            project(c, LONG[1], AT[1] + (c - 1) * LONG[1])
            return carry

        lax.fori_loop(1, 3, project_rest, 0)
        for c in range(3):
            own = pl.ds(AT[c], LONG[c])
            pltpu.make_async_copy(y_s.at[own], y.at[own], y_sem.at[c]).wait()

    pl.run_scoped(back, pltpu.VMEM((N * HEAD, D), jnp.bfloat16))

    for unit in LEFT:
        sent(unit)
    for c in range(3):
        part = ostage.at[pl.ds(0, 15 * LONG[c])]
        pltpu.make_async_copy(part, part, o_send.at[c]).wait()


def solution(mesh):
    def step(x, gain, wq, wk, wv, wo):
        half = HEAD // 2
        rate = float(THETA) ** (-np.arange(half) / half)
        table = lambda place: jnp.asarray(np.concatenate([f(place[:, None] * rate) for f in (np.cos, np.sin)], 1), jnp.float32)
        order = jnp.asarray(np.broadcast_to(TOKENS[:, None], (OWN, W)), jnp.int32)
        vmem, any_ = pl.BlockSpec(memory_space=pltpu.VMEM), pl.BlockSpec(memory_space=pl.ANY)
        bf, f32 = jnp.bfloat16, jnp.float32
        dma = pltpu.SemaphoreType.DMA
        return pl.pallas_call(
            kernel,
            out_shape=jax.ShapeDtypeStruct((OWN, D), bf),
            in_specs=[vmem] * 4 + [any_] * 5,
            out_specs=any_,
            scratch_shapes=[
                pltpu.VMEM((OWN, D), bf), pltpu.VMEM((OWN, D), bf), pltpu.VMEM((2 * OWN, half), f32), pltpu.VMEM((2 * OWN, half), f32),
                pltpu.VMEM((2 * OWN, D), bf), pltpu.VMEM((3, N * OWN, HEAD), bf), pltpu.VMEM((3, N * OWN, HEAD), bf),
                pltpu.VMEM((HEAD + 8, N * OWN), bf), pltpu.VMEM((N * OWN, HEAD), bf), pltpu.VMEM((OWN, N * HEAD), bf),
                dma((SLOTS,)), dma((4,)), dma, dma((3,)), dma((3,)), dma((3,)), dma((6, COUNT)), dma((5,)), dma((3,)), dma((3,)),
            ],
            compiler_params=pltpu.CompilerParams(collective_id=0, has_side_effects=True, vmem_limit_bytes=67_043_328),
            name="layer",
        )(gain, table(TOKENS), table(np.arange(N) * OWN)[:, None], order, x, wq, wk, wv, wo)

    tokens, whole = P(("dp", "sp"), None), P(None, None)
    return jax.shard_map(step, mesh=mesh, in_specs=(tokens, P(None), whole, whole, whole, whole), out_specs=tokens, check_vma=False)
```

```python
import jax
import jax.numpy as jnp
import numpy as np
from jax import lax
from jax.experimental import pallas as pl
from jax.experimental.pallas import tpu as pltpu
from jax.sharding import PartitionSpec as P

HEAD = 256
THETA = 10000
LOG2E = 1.4426950408889634
HIDDEN = -1e30
MESH = pl.DeviceIdType.MESH
OWN = 256
N = 16
D = 3072
BITS = (8, 4, 2)
PIECES = ((32, 32, 32), (32, 32, 16), (32, 16, 32))
ROWS = tuple(sum(p) for p in PIECES)
OFF = tuple(sum(ROWS[:g]) for g in range(3))
LONG = tuple(sum(p[c] for p in PIECES) for c in range(3))
AT = tuple(sum(LONG[:c]) for c in range(3))
ORDER = (8, 4, 2, 12, 6, 10, 0)
SLOTS = 4
W = 256
WINDOWS = (20, 20, 20, 20, 40, 40)


def turn(me, r):
    out = me
    for b in (8, 4, 2, 1):
        if r & b:
            out = out + b * (1 - 2 * lax.rem(lax.div(me, b), 2))
    return out


def groups(r):
    return [g for g in range(3) if not r & BITS[g]]


def height(r):
    return 2 * sum(ROWS[g] for g in groups(r))


def stage_at(r):
    return sum(2 * height(s) for s in ORDER[: ORDER.index(r)])


def token(g, c):
    return AT[c] + sum(PIECES[h][c] for h in range(g))


def inside(g, c):
    return sum(PIECES[g][:c])


TOKENS = np.concatenate([token(g, c) + np.arange(PIECES[g][c]) for g in range(3) for c in range(3)])


def dot(a, b, ca, cb):
    return lax.dot_general(a, b, (((ca,), (cb,)), ((), ())), preferred_element_type=jnp.float32)


def al(x):
    return pl.multiple_of(x, 16)


def attend_strip(rows, first, s, q, k_ref, vt, order_ref):
    lo, hi = s * W // rows, (s * W + W - 1) // rows
    clear, keys = lo * OWN, (hi + 1) * OWN
    col = s * W + lax.broadcasted_iota(jnp.int32, (1, W), 1)
    place = sum(jnp.where(col >= i * rows, OWN - rows, 0) for i in range(lo + 1, hi + 1)) + (lo * (OWN - rows) + first) + col
    x = dot(k_ref[clear:keys, :], q, 1, 1)
    x = jnp.concatenate(
        [jnp.where(order_ref[...] <= place - (lo + n) * OWN, x[n * OWN : (n + 1) * OWN], HIDDEN) for n in range(hi - lo + 1)], axis=0)
    if clear:
        x = jnp.concatenate([dot(k_ref[:clear, :], q, 1, 1), x], axis=0)
    top = x.max(axis=0, keepdims=True)
    p = jnp.exp2((x - top) * (HEAD**-0.5 * LOG2E)).astype(jnp.bfloat16)
    acc = dot(vt[:, :keys], p, 1, 0)
    out = acc[:HEAD] * (1 / acc[HEAD : HEAD + 1])
    return out.T.astype(jnp.bfloat16)


def rows_of(phase, i):
    r = ORDER[i]
    heads = 2 if r else 1
    if phase < 3:
        return heads * sum(ROWS[g] for g in groups(r)) * (2 if phase == 2 else 1)
    return heads * 2 * sum(PIECES[g][phase - 3] for g in groups(r))


COUNT = len(ORDER)
UNITS = [(phase, i) for phase in range(6) for i in range(COUNT) if rows_of(phase, i)]
BEFORE = {}
seen = 0
for at, unit in enumerate(UNITS):
    BEFORE[unit] = UNITS[seen : max(at - WINDOWS[unit[0]], seen)]
    seen += len(BEFORE[unit])
LEFT = UNITS[seen:]


def kernel(gain_ref, turn_ref, base_ref, order_ref, x, wq, wk, wv, wo, y,
           x_s, y_s, cos_s, sin_s, a_s, stage, land, vt, ostage, oland,
           w_sem, wo_sem, x_sem, y_sem, x_send, x_recv, t_send, t_recv, o_send, o_recv):
    me = lax.axis_index("sp")
    side = lax.rem(me, 2)
    weights = (wv, wk, wq)

    read = pltpu.make_async_copy(x, x_s, x_sem)
    read.start()
    barrier = pltpu.get_barrier_semaphore()
    for r in range(1, N):
        pl.semaphore_signal(barrier, inc=1, device_id=(0, turn(me, r)), device_id_type=MESH)

    def blocks(t, owner, g):
        if t < 2:
            return [(0, ROWS[g], al(owner * OWN + OFF[g]), None)]
        return [(inside(g, c), PIECES[g][c], al(N * AT[c] + owner * LONG[c] + token(g, c) - AT[c]), c) for c in range(3)]

    def sent(unit):
        part = stage.at[0, pl.ds(0, rows_of(*unit))]
        pltpu.make_async_copy(part, part, t_send.at[unit[0], unit[1]]).wait()

    def send(phase, i):
        if not rows_of(phase, i):
            return
        for unit in BEFORE[phase, i]:
            sent(unit)
        r, t = ORDER[i], (0, 0, 1, 2, 2, 2)[phase]
        for p in range(2 if r else 1):
            at = stage_at(r) + (p if r else 1 - side) * height(r)
            to = turn(me, r) - side + p if r else turn(me, 1)
            for g in groups(r):
                for n, owner in enumerate((me, turn(me, BITS[g]))):
                    for skip, rows, to_row, c in blocks(t, owner, g):
                        if phase < 2 and n == phase or phase == 2 or phase > 2 and phase - 3 == c:
                            pltpu.make_async_remote_copy(
                                src_ref=stage.at[t, pl.ds(al(at + skip), rows)], dst_ref=land.at[t, pl.ds(to_row, rows)],
                                send_sem=t_send.at[phase, i], recv_sem=t_recv.at[t + max(phase - 3, 0)], device_id=(0, to),
                                device_id_type=MESH).start()
                    at += ROWS[g]

    def front(w_s):
        def fetch(step, i, slot):
            head = pl.multiple_of((turn(me, ORDER[i]) - side) * HEAD, 2 * HEAD)
            for k, is_k in enumerate((step < 2, step == 2, step == 3)):
                @pl.when(is_k)
                def _(k=k):
                    pltpu.make_async_copy(weights[k].at[:, pl.ds(head, 2 * HEAD)], w_s.at[slot], w_sem.at[slot]).start()

        for i in range(SLOTS - 1):
            fetch(jnp.int32(0), i, i)

        def swap(g):
            base = 2 * OFF[g]
            return pltpu.make_async_remote_copy(
                src_ref=a_s.at[pl.ds(base, ROWS[g])], dst_ref=a_s.at[pl.ds(base + ROWS[g], ROWS[g])],
                send_sem=x_send.at[g], recv_sem=x_recv.at[g], device_id=(0, turn(me, BITS[g])), device_id_type=MESH)

        gain = gain_ref[...].astype(jnp.float32).reshape(1, D)
        read.wait()
        for g in range(3):
            for n in range(ROWS[g] // 16):
                at = int(TOKENS[OFF[g] + n * 16])
                wide = x_s[at : at + 16, :].astype(jnp.float32)
                scale = lax.rsqrt(jnp.mean(wide * wide, -1, keepdims=True) + 1e-6)
                a_s[2 * OFF[g] + n * 16 : 2 * OFF[g] + n * 16 + 16, :] = (wide * scale * gain).astype(jnp.bfloat16)
            if g == 0:
                pl.semaphore_wait(barrier, N - 1)
            else:
                swap(g - 1).start()
        swap(2).start()

        for g in range(3):
            for n, owner in enumerate((me, turn(me, BITS[g]))):
                cb, sb = base_ref[owner, :, : HEAD // 2], base_ref[owner, :, HEAD // 2 :]
                ct, st = turn_ref[OFF[g] : OFF[g] + ROWS[g], : HEAD // 2], turn_ref[OFF[g] : OFF[g] + ROWS[g], HEAD // 2 :]
                at = slice(2 * OFF[g] + n * ROWS[g], 2 * OFF[g] + (n + 1) * ROWS[g])
                cos_s[at, :] = cb * ct - sb * st
                sin_s[at, :] = sb * ct + cb * st

        def next_weights(step, i):
            n = step * COUNT + i
            slot = lax.rem(n, SLOTS)
            pltpu.make_async_copy(wk.at[:, pl.ds(0, 2 * HEAD)], w_s.at[slot], w_sem.at[slot]).wait()
            ahead = i + SLOTS - 1
            fetch(step + ahead // COUNT, ahead % COUNT, lax.rem(n + SLOTS - 1, SLOTS))
            return w_s[slot]

        def rotated(y, cos, sin):
            u, v = y[:, : HEAD // 2], y[:, HEAD // 2 :]
            return jnp.concatenate([u * cos - v * sin, v * cos + u * sin], 1).astype(jnp.bfloat16)

        def half(which, carry):
            @pl.when(which == 1)
            def _():
                for g in range(3):
                    swap(g).wait()

            def sends(i):
                for k in range(2):
                    @pl.when(which == k)
                    def _(k=k):
                        send(k, i)

            for i, r in enumerate(ORDER):
                w = next_weights(which, i)
                if i > 0:
                    sends(i - 1)
                rows = lambda ref: jnp.concatenate(
                    [ref[pl.ds(al(2 * OFF[g] + which * ROWS[g]), ROWS[g]), :] for g in groups(r)], axis=0)
                y = dot(rows(a_s), w, 1, 0).astype(jnp.bfloat16)
                for p in range(2):
                    z = y[:, p * HEAD : (p + 1) * HEAD]
                    at, n = stage_at(r) + p * height(r), 0
                    for g in groups(r):
                        stage[0, pl.ds(al(at + which * ROWS[g]), ROWS[g]), :] = z[n : n + ROWS[g]]
                        at, n = at + 2 * ROWS[g], n + ROWS[g]
            sends(COUNT - 1)
            return carry

        lax.fori_loop(0, 2, half, 0)

        def project(t, carry):
            def sends(i):
                for k in (1, 2):
                    @pl.when(t == k)
                    def _(k=k):
                        send(k + 1, i)

            for i, r in enumerate(ORDER):
                w = next_weights(t + 1, i)
                if i > 0:
                    sends(i - 1)
                cuts = [slice(2 * OFF[g], 2 * OFF[g] + 2 * ROWS[g]) for g in groups(r)]
                rows = lambda ref: jnp.concatenate([ref[c, :] for c in cuts], axis=0)
                y = dot(rows(a_s), w, 1, 0).astype(jnp.bfloat16).astype(jnp.float32)
                cos, sin = rows(cos_s), rows(sin_s)
                for p in range(2):
                    at = stage_at(r) + p * height(r)
                    stage[t, at : at + height(r), :] = rotated(y[:, p * HEAD : (p + 1) * HEAD], cos, sin)
            sends(COUNT - 1)
            return carry

        lax.fori_loop(1, 3, project, 0)

    pl.run_scoped(front, pltpu.VMEM((SLOTS, D, 2 * HEAD), jnp.bfloat16))

    def back(wo_s):
        for i in range(COUNT):
            send(4, i)

        def load(i):
            return pltpu.make_async_copy(wo.at[pl.ds(i * 1024, 1024)], wo_s.at[pl.ds(i * 1024, 1024)], wo_sem.at[i])

        for i in range(4):
            load(i).start()

        def arrived(t, sem, rows):
            pltpu.make_async_copy(land.at[t, pl.ds(0, rows)], land.at[t, pl.ds(0, rows)], t_recv.at[sem]).wait()

        for t in range(3):
            at = stage_at(0) + side * height(0)
            for g in range(3):
                for owner in (me, turn(me, BITS[g])):
                    for skip, rows, to_row, _ in blocks(t, owner, g):
                        land[t, pl.ds(to_row, rows), :] = stage[t, pl.ds(al(at + skip), rows), :]
                    at += ROWS[g]
        vt[HEAD:, :] = jnp.ones((8, N * OWN), jnp.bfloat16)
        arrived(0, 0, 14 * OWN)
        for j in range(N):
            vt[:HEAD, j * OWN : (j + 1) * OWN] = land[0, j * OWN : (j + 1) * OWN, :].T
        arrived(1, 1, 14 * OWN)

        mine = pl.ds(pl.multiple_of(me * HEAD, HEAD), HEAD)

        def attend(c, rows, first, between):
            arrived(2, 2 + c, 14 * rows)

            def give(half):
                for r in (4, 2, 6, 5, 3, 7, 1, 0):
                    to = turn(me, r) + 8 * (half - lax.div(me, 8))

                    @pl.when(me != to)
                    def _(to=to):
                        pltpu.make_async_remote_copy(
                            src_ref=ostage.at[pl.ds(al(N * first + to * rows), rows)], dst_ref=oland.at[pl.ds(al(first), rows), mine],
                            send_sem=o_send.at[c], recv_sem=o_recv.at[c], device_id=(0, to), device_id_type=MESH).start()

            for s in range(N * rows // W):
                at = pl.ds(al(N * first + s * W), W)
                ostage[at, :] = attend_strip(rows, first, s, land[2, at, :], land.at[1], vt, order_ref)
                between(s)
                if s == 2:
                    give(0)
            give(1)
            oland[pl.ds(al(first), rows), mine] = ostage[pl.ds(al(N * first + me * rows), rows), :]

        def last_queries(s):
            for i in range(COUNT * s // 5, min(COUNT * (s + 1) // 5, COUNT)):
                send(5, i)

        attend(0, LONG[0], 0, last_queries)

        def rest(c, carry):
            attend(c, LONG[1], AT[1] + (c - 1) * LONG[1], lambda s: None)
            return carry

        lax.fori_loop(1, 3, rest, 0)

        for i in range(4):
            load(i).wait()

        def project(c, rows, first):
            part = ostage.at[pl.ds(0, 15 * rows)]
            pltpu.make_async_copy(part, part, o_recv.at[c]).wait()
            own = pl.ds(al(first), rows)

            def out(n, carry):
                cols = pl.ds(pl.multiple_of(n * 1024, 1024), 1024)
                z = dot(oland[own, :], wo_s[:, cols], 1, 0)
                y_s[own, cols] = (x_s[own, cols].astype(jnp.float32) + z).astype(jnp.bfloat16)
                return carry

            lax.fori_loop(0, D // 1024, out, 0)
            pltpu.make_async_copy(y_s.at[own], y.at[own], y_sem.at[c]).start()

        project(0, LONG[0], 0)

        def project_rest(c, carry):
            project(c, LONG[1], AT[1] + (c - 1) * LONG[1])
            return carry

        lax.fori_loop(1, 3, project_rest, 0)
        for c in range(3):
            own = pl.ds(AT[c], LONG[c])
            pltpu.make_async_copy(y_s.at[own], y.at[own], y_sem.at[c]).wait()

    pl.run_scoped(back, pltpu.VMEM((N * HEAD, D), jnp.bfloat16))

    for unit in LEFT:
        sent(unit)
    for c in range(3):
        part = ostage.at[pl.ds(0, 15 * LONG[c])]
        pltpu.make_async_copy(part, part, o_send.at[c]).wait()


def solution(mesh):
    def step(x, gain, wq, wk, wv, wo):
        half = HEAD // 2
        rate = float(THETA) ** (-np.arange(half) / half)
        table = lambda place: jnp.asarray(np.concatenate([f(place[:, None] * rate) for f in (np.cos, np.sin)], 1), jnp.float32)
        order = jnp.asarray(np.broadcast_to(TOKENS[:, None], (OWN, W)), jnp.int32)
        vmem, any_ = pl.BlockSpec(memory_space=pltpu.VMEM), pl.BlockSpec(memory_space=pl.ANY)
        bf, f32 = jnp.bfloat16, jnp.float32
        dma = pltpu.SemaphoreType.DMA
        return pl.pallas_call(
            kernel,
            out_shape=jax.ShapeDtypeStruct((OWN, D), bf),
            in_specs=[vmem] * 4 + [any_] * 5,
            out_specs=any_,
            scratch_shapes=[
                pltpu.VMEM((OWN, D), bf), pltpu.VMEM((OWN, D), bf), pltpu.VMEM((2 * OWN, half), f32), pltpu.VMEM((2 * OWN, half), f32),
                pltpu.VMEM((2 * OWN, D), bf), pltpu.VMEM((3, N * OWN, HEAD), bf), pltpu.VMEM((3, N * OWN, HEAD), bf),
                pltpu.VMEM((HEAD + 8, N * OWN), bf), pltpu.VMEM((N * OWN, HEAD), bf), pltpu.VMEM((OWN, N * HEAD), bf),
                dma((SLOTS,)), dma((4,)), dma, dma((3,)), dma((3,)), dma((3,)), dma((6, COUNT)), dma((5,)), dma((3,)), dma((3,)),
            ],
            compiler_params=pltpu.CompilerParams(collective_id=0, has_side_effects=True, vmem_limit_bytes=67_043_328),
            name="layer",
        )(gain, table(TOKENS), table(np.arange(N) * OWN)[:, None], order, x, wq, wk, wv, wo)

    tokens, whole = P(("dp", "sp"), None), P(None, None)
    return jax.shard_map(step, mesh=mesh, in_specs=(tokens, P(None), whole, whole, whole, whole), out_specs=tokens, check_vma=False)
```

```python
import jax
import jax.numpy as jnp
import numpy as np
from jax import lax
from jax.experimental import pallas as pl
from jax.experimental.pallas import tpu as pltpu
from jax.sharding import PartitionSpec as P

HEAD = 256
THETA = 10000
LOG2E = 1.4426950408889634
HIDDEN = -1e30
MESH = pl.DeviceIdType.MESH
OWN = 256
N = 16
D = 3072
BITS = (8, 4, 2)
PIECES = ((32, 32, 32), (16, 32, 32), (16, 32, 32))
ROWS = tuple(sum(p) for p in PIECES)
OFF = tuple(sum(ROWS[:g]) for g in range(3))
LONG = tuple(sum(p[c] for p in PIECES) for c in range(3))
AT = tuple(sum(LONG[:c]) for c in range(3))
ORDER = (8, 4, 2, 12, 6, 10, 0)
SLOTS = 4
W = 256
WINDOWS = (20, 20, 20, 20, 40, 40)


def turn(me, r):
    out = me
    for b in (8, 4, 2, 1):
        if r & b:
            out = out + b * (1 - 2 * lax.rem(lax.div(me, b), 2))
    return out


def groups(r):
    return [g for g in range(3) if not r & BITS[g]]


def height(r):
    return 2 * sum(ROWS[g] for g in groups(r))


def stage_at(r):
    return sum(2 * height(s) for s in ORDER[: ORDER.index(r)])


def token(g, c):
    return AT[c] + sum(PIECES[h][c] for h in range(g))


def inside(g, c):
    return sum(PIECES[g][:c])


TOKENS = np.concatenate([token(g, c) + np.arange(PIECES[g][c]) for g in range(3) for c in range(3)])


def dot(a, b, ca, cb):
    return lax.dot_general(a, b, (((ca,), (cb,)), ((), ())), preferred_element_type=jnp.float32)


def al(x):
    return pl.multiple_of(x, 16)


def attend_strip(rows, first, s, q, k_ref, vt, order_ref):
    lo, hi = s * W // rows, (s * W + W - 1) // rows
    clear, keys = lo * OWN, (hi + 1) * OWN
    col = s * W + lax.broadcasted_iota(jnp.int32, (1, W), 1)
    place = sum(jnp.where(col >= i * rows, OWN - rows, 0) for i in range(lo + 1, hi + 1)) + (lo * (OWN - rows) + first) + col
    x = dot(k_ref[clear:keys, :], q, 1, 1)
    x = jnp.concatenate(
        [jnp.where(order_ref[...] <= place - (lo + n) * OWN, x[n * OWN : (n + 1) * OWN], HIDDEN) for n in range(hi - lo + 1)], axis=0)
    if clear:
        x = jnp.concatenate([dot(k_ref[:clear, :], q, 1, 1), x], axis=0)
    top = x.max(axis=0, keepdims=True)
    p = jnp.exp2((x - top) * (HEAD**-0.5 * LOG2E)).astype(jnp.bfloat16)
    acc = dot(vt[:, :keys], p, 1, 0)
    out = acc[:HEAD] * (1 / acc[HEAD : HEAD + 1])
    return out.T.astype(jnp.bfloat16)


def rows_of(phase, i):
    r = ORDER[i]
    heads = 2 if r else 1
    if phase < 3:
        return heads * sum(ROWS[g] for g in groups(r)) * (2 if phase == 2 else 1)
    return heads * 2 * sum(PIECES[g][phase - 3] for g in groups(r))


COUNT = len(ORDER)
UNITS = [(phase, i) for phase in range(6) for i in range(COUNT) if rows_of(phase, i)]
BEFORE = {}
seen = 0
for at, unit in enumerate(UNITS):
    BEFORE[unit] = UNITS[seen : max(at - WINDOWS[unit[0]], seen)]
    seen += len(BEFORE[unit])
LEFT = UNITS[seen:]


def kernel(gain_ref, turn_ref, base_ref, order_ref, x, wq, wk, wv, wo, y,
           x_s, y_s, cos_s, sin_s, a_s, stage, land, vt, ostage, oland,
           w_sem, wo_sem, x_sem, y_sem, x_send, x_recv, t_send, t_recv, o_send, o_recv):
    me = lax.axis_index("sp")
    side = lax.rem(me, 2)
    weights = (wv, wk, wq)

    read = pltpu.make_async_copy(x, x_s, x_sem)
    read.start()
    barrier = pltpu.get_barrier_semaphore()
    for r in range(1, N):
        pl.semaphore_signal(barrier, inc=1, device_id=(0, turn(me, r)), device_id_type=MESH)

    def blocks(t, owner, g):
        if t < 2:
            return [(0, ROWS[g], al(owner * OWN + OFF[g]), None)]
        return [(inside(g, c), PIECES[g][c], al(N * AT[c] + owner * LONG[c] + token(g, c) - AT[c]), c) for c in range(3)]

    def sent(unit):
        part = stage.at[0, pl.ds(0, rows_of(*unit))]
        pltpu.make_async_copy(part, part, t_send.at[unit[0], unit[1]]).wait()

    def send(phase, i):
        if not rows_of(phase, i):
            return
        for unit in BEFORE[phase, i]:
            sent(unit)
        r, t = ORDER[i], (0, 0, 1, 2, 2, 2)[phase]
        for p in range(2 if r else 1):
            at = stage_at(r) + (p if r else 1 - side) * height(r)
            to = turn(me, r) - side + p if r else turn(me, 1)
            for g in groups(r):
                for n, owner in enumerate((me, turn(me, BITS[g]))):
                    for skip, rows, to_row, c in blocks(t, owner, g):
                        if phase < 2 and n == phase or phase == 2 or phase > 2 and phase - 3 == c:
                            pltpu.make_async_remote_copy(
                                src_ref=stage.at[t, pl.ds(al(at + skip), rows)], dst_ref=land.at[t, pl.ds(to_row, rows)],
                                send_sem=t_send.at[phase, i], recv_sem=t_recv.at[t + max(phase - 3, 0)], device_id=(0, to),
                                device_id_type=MESH).start()
                    at += ROWS[g]

    def front(w_s):
        def fetch(step, i, slot):
            head = pl.multiple_of((turn(me, ORDER[i]) - side) * HEAD, 2 * HEAD)
            for k, is_k in enumerate((step < 2, step == 2, step == 3)):
                @pl.when(is_k)
                def _(k=k):
                    pltpu.make_async_copy(weights[k].at[:, pl.ds(head, 2 * HEAD)], w_s.at[slot], w_sem.at[slot]).start()

        for i in range(SLOTS - 1):
            fetch(jnp.int32(0), i, i)

        def swap(g):
            base = 2 * OFF[g]
            return pltpu.make_async_remote_copy(
                src_ref=a_s.at[pl.ds(base, ROWS[g])], dst_ref=a_s.at[pl.ds(base + ROWS[g], ROWS[g])],
                send_sem=x_send.at[g], recv_sem=x_recv.at[g], device_id=(0, turn(me, BITS[g])), device_id_type=MESH)

        gain = gain_ref[...].astype(jnp.float32).reshape(1, D)
        read.wait()
        for g in range(3):
            for n in range(ROWS[g] // 16):
                at = int(TOKENS[OFF[g] + n * 16])
                wide = x_s[at : at + 16, :].astype(jnp.float32)
                scale = lax.rsqrt(jnp.mean(wide * wide, -1, keepdims=True) + 1e-6)
                a_s[2 * OFF[g] + n * 16 : 2 * OFF[g] + n * 16 + 16, :] = (wide * scale * gain).astype(jnp.bfloat16)
            if g == 0:
                pl.semaphore_wait(barrier, N - 1)
            else:
                swap(g - 1).start()
        swap(2).start()

        for g in range(3):
            for n, owner in enumerate((me, turn(me, BITS[g]))):
                cb, sb = base_ref[owner, :, : HEAD // 2], base_ref[owner, :, HEAD // 2 :]
                ct, st = turn_ref[OFF[g] : OFF[g] + ROWS[g], : HEAD // 2], turn_ref[OFF[g] : OFF[g] + ROWS[g], HEAD // 2 :]
                at = slice(2 * OFF[g] + n * ROWS[g], 2 * OFF[g] + (n + 1) * ROWS[g])
                cos_s[at, :] = cb * ct - sb * st
                sin_s[at, :] = sb * ct + cb * st

        def next_weights(step, i):
            n = step * COUNT + i
            slot = lax.rem(n, SLOTS)
            pltpu.make_async_copy(wk.at[:, pl.ds(0, 2 * HEAD)], w_s.at[slot], w_sem.at[slot]).wait()
            ahead = i + SLOTS - 1
            fetch(step + ahead // COUNT, ahead % COUNT, lax.rem(n + SLOTS - 1, SLOTS))
            return w_s[slot]

        def rotated(y, cos, sin):
            u, v = y[:, : HEAD // 2], y[:, HEAD // 2 :]
            return jnp.concatenate([u * cos - v * sin, v * cos + u * sin], 1).astype(jnp.bfloat16)

        def half(which, carry):
            @pl.when(which == 1)
            def _():
                for g in range(3):
                    swap(g).wait()

            def sends(i):
                for k in range(2):
                    @pl.when(which == k)
                    def _(k=k):
                        send(k, i)

            for i, r in enumerate(ORDER):
                w = next_weights(which, i)
                if i > 0:
                    sends(i - 1)
                rows = lambda ref: jnp.concatenate(
                    [ref[pl.ds(al(2 * OFF[g] + which * ROWS[g]), ROWS[g]), :] for g in groups(r)], axis=0)
                y = dot(rows(a_s), w, 1, 0).astype(jnp.bfloat16)
                for p in range(2):
                    z = y[:, p * HEAD : (p + 1) * HEAD]
                    at, n = stage_at(r) + p * height(r), 0
                    for g in groups(r):
                        stage[0, pl.ds(al(at + which * ROWS[g]), ROWS[g]), :] = z[n : n + ROWS[g]]
                        at, n = at + 2 * ROWS[g], n + ROWS[g]
            sends(COUNT - 1)
            return carry

        lax.fori_loop(0, 2, half, 0)

        def project(t, carry):
            def sends(i):
                for k in (1, 2):
                    @pl.when(t == k)
                    def _(k=k):
                        send(k + 1, i)

            for i, r in enumerate(ORDER):
                w = next_weights(t + 1, i)
                if i > 0:
                    sends(i - 1)
                cuts = [slice(2 * OFF[g], 2 * OFF[g] + 2 * ROWS[g]) for g in groups(r)]
                rows = lambda ref: jnp.concatenate([ref[c, :] for c in cuts], axis=0)
                y = dot(rows(a_s), w, 1, 0).astype(jnp.bfloat16).astype(jnp.float32)
                cos, sin = rows(cos_s), rows(sin_s)
                for p in range(2):
                    at = stage_at(r) + p * height(r)
                    stage[t, at : at + height(r), :] = rotated(y[:, p * HEAD : (p + 1) * HEAD], cos, sin)
            sends(COUNT - 1)
            return carry

        lax.fori_loop(1, 3, project, 0)

    pl.run_scoped(front, pltpu.VMEM((SLOTS, D, 2 * HEAD), jnp.bfloat16))

    def back(wo_s):
        for i in range(COUNT):
            send(4, i)

        def load(i):
            return pltpu.make_async_copy(wo.at[pl.ds(i * 1024, 1024)], wo_s.at[pl.ds(i * 1024, 1024)], wo_sem.at[i])

        for i in range(4):
            load(i).start()

        def arrived(t, sem, rows):
            pltpu.make_async_copy(land.at[t, pl.ds(0, rows)], land.at[t, pl.ds(0, rows)], t_recv.at[sem]).wait()

        for t in range(3):
            at = stage_at(0) + side * height(0)
            for g in range(3):
                for owner in (me, turn(me, BITS[g])):
                    for skip, rows, to_row, _ in blocks(t, owner, g):
                        land[t, pl.ds(to_row, rows), :] = stage[t, pl.ds(al(at + skip), rows), :]
                    at += ROWS[g]
        vt[HEAD:, :] = jnp.ones((8, N * OWN), jnp.bfloat16)
        arrived(0, 0, 14 * OWN)
        for j in range(N):
            vt[:HEAD, j * OWN : (j + 1) * OWN] = land[0, j * OWN : (j + 1) * OWN, :].T
        arrived(1, 1, 14 * OWN)

        mine = pl.ds(pl.multiple_of(me * HEAD, HEAD), HEAD)

        def attend(c, rows, first, between):
            arrived(2, 2 + c, 14 * rows)

            def give(half):
                for r in (4, 2, 6, 5, 3, 7, 1, 0):
                    to = turn(me, r) + 8 * (half - lax.div(me, 8))

                    @pl.when(me != to)
                    def _(to=to):
                        pltpu.make_async_remote_copy(
                            src_ref=ostage.at[pl.ds(al(N * first + to * rows), rows)], dst_ref=oland.at[pl.ds(al(first), rows), mine],
                            send_sem=o_send.at[c], recv_sem=o_recv.at[c], device_id=(0, to), device_id_type=MESH).start()

            for s in range(N * rows // W):
                at = pl.ds(al(N * first + s * W), W)
                ostage[at, :] = attend_strip(rows, first, s, land[2, at, :], land.at[1], vt, order_ref)
                between(s)
                if s == 2:
                    give(0)
            give(1)
            oland[pl.ds(al(first), rows), mine] = ostage[pl.ds(al(N * first + me * rows), rows), :]

        def last_queries(s):
            for i in range(COUNT * s // 4, COUNT * (s + 1) // 4):
                send(5, i)

        attend(0, LONG[0], 0, last_queries)

        def rest(c, carry):
            attend(c, LONG[1], AT[1] + (c - 1) * LONG[1], lambda s: None)
            return carry

        lax.fori_loop(1, 3, rest, 0)

        for i in range(4):
            load(i).wait()

        def project(c, rows, first):
            part = ostage.at[pl.ds(0, 15 * rows)]
            pltpu.make_async_copy(part, part, o_recv.at[c]).wait()
            own = pl.ds(al(first), rows)

            def out(n, carry):
                cols = pl.ds(pl.multiple_of(n * 1024, 1024), 1024)
                z = dot(oland[own, :], wo_s[:, cols], 1, 0)
                y_s[own, cols] = (x_s[own, cols].astype(jnp.float32) + z).astype(jnp.bfloat16)
                return carry

            lax.fori_loop(0, D // 1024, out, 0)
            pltpu.make_async_copy(y_s.at[own], y.at[own], y_sem.at[c]).start()

        project(0, LONG[0], 0)

        def project_rest(c, carry):
            project(c, LONG[1], AT[1] + (c - 1) * LONG[1])
            return carry

        lax.fori_loop(1, 3, project_rest, 0)
        for c in range(3):
            own = pl.ds(AT[c], LONG[c])
            pltpu.make_async_copy(y_s.at[own], y.at[own], y_sem.at[c]).wait()

    pl.run_scoped(back, pltpu.VMEM((N * HEAD, D), jnp.bfloat16))

    for unit in LEFT:
        sent(unit)
    for c in range(3):
        part = ostage.at[pl.ds(0, 15 * LONG[c])]
        pltpu.make_async_copy(part, part, o_send.at[c]).wait()


def solution(mesh):
    def step(x, gain, wq, wk, wv, wo):
        half = HEAD // 2
        rate = float(THETA) ** (-np.arange(half) / half)
        table = lambda place: jnp.asarray(np.concatenate([f(place[:, None] * rate) for f in (np.cos, np.sin)], 1), jnp.float32)
        order = jnp.asarray(np.broadcast_to(TOKENS[:, None], (OWN, W)), jnp.int32)
        vmem, any_ = pl.BlockSpec(memory_space=pltpu.VMEM), pl.BlockSpec(memory_space=pl.ANY)
        bf, f32 = jnp.bfloat16, jnp.float32
        dma = pltpu.SemaphoreType.DMA
        return pl.pallas_call(
            kernel,
            out_shape=jax.ShapeDtypeStruct((OWN, D), bf),
            in_specs=[vmem] * 4 + [any_] * 5,
            out_specs=any_,
            scratch_shapes=[
                pltpu.VMEM((OWN, D), bf), pltpu.VMEM((OWN, D), bf), pltpu.VMEM((2 * OWN, half), f32), pltpu.VMEM((2 * OWN, half), f32),
                pltpu.VMEM((2 * OWN, D), bf), pltpu.VMEM((3, N * OWN, HEAD), bf), pltpu.VMEM((3, N * OWN, HEAD), bf),
                pltpu.VMEM((HEAD + 8, N * OWN), bf), pltpu.VMEM((N * OWN, HEAD), bf), pltpu.VMEM((OWN, N * HEAD), bf),
                dma((SLOTS,)), dma((4,)), dma, dma((3,)), dma((3,)), dma((3,)), dma((6, COUNT)), dma((5,)), dma((3,)), dma((3,)),
            ],
            compiler_params=pltpu.CompilerParams(collective_id=0, has_side_effects=True, vmem_limit_bytes=67_043_328),
            name="layer",
        )(gain, table(TOKENS), table(np.arange(N) * OWN)[:, None], order, x, wq, wk, wv, wo)

    tokens, whole = P(("dp", "sp"), None), P(None, None)
    return jax.shard_map(step, mesh=mesh, in_specs=(tokens, P(None), whole, whole, whole, whole), out_specs=tokens, check_vma=False)
```
